32 devices in a mesh: seq: 16 (over z, x, core), head: 2 (over y).
Axes of the slice: x: 2, y: 2, z: 4, core: 2. Of those that a mesh axis runs over, the one named last changes fastest.
Arguments:
- query: bfloat16 [8192, 1024], P('seq', 'head'), may hold values from -6 to 6
- key_rows: bfloat16 [8192, 128], P('seq'), may hold values from -6 to 6
- value_rows: bfloat16 [8192, 128], P('seq'), may hold values from -6 to 6
- output: bfloat16 [8192, 1024], P('seq', 'head'), may hold values from -1.5 to 1.5
- grad_output: bfloat16 [8192, 1024], P('seq', 'head'), may hold values from -144 to 144
- log_norm: float32 [8, 8192], P('head', 'seq'), may hold values from 0.5 to 12
- stripe: int32 [16], replicated, may hold values from 0 to 15, each once
Outputs:
- grad_query: bfloat16 [8192, 1024], P('seq', 'head')
- grad_key: bfloat16 [8192, 128], P(('seq', 'head'))
- grad_value: bfloat16 [8192, 128], P(('seq', 'head'))
The draws below stay inside these ranges and needn't reach their ends.
Inputs may be any that keep to these rules, and one draw needn't show every extreme that they name: stripe is a permutation of 0 to 15.
All inputs are finite; a program needn't handle non-finite values.
Results may differ from the reference program's by a relative error of at most 0.0051.
Values may be sent and summed in bfloat16 or wider, within the bound.
A program may use at most 192 MiB of HBM per device.

```python
import jax
import jax.numpy as jnp
from jax import lax

DH = 128
QH = 8
WINDOW = 8
S_DEV = 512
LEN = 8192
N_SEQ = 16


def draw_log_norm(key, part):
    local_row = (jnp.arange(LEN) % S_DEV).astype(jnp.float32)
    counts = WINDOW * (local_row + 0.5)
    base_level = jnp.log(counts) + 0.5
    jitter = jax.random.normal(key, (QH, LEN), jnp.float32) * 0.2
    return jnp.clip(base_level[None, :] + jitter, 0.5, 12.0).astype(jnp.float32)


def shard_levels(stream_key, shape, cuts, least, top_value):
    def one(position, parts):
        steps = jax.random.uniform(jax.random.fold_in(jax.random.fold_in(stream_key, 6), position), (parts,), jnp.float32, least / len(cuts), top_value / len(cuts))
        return jnp.repeat(jnp.exp(steps), shape[position] // parts).reshape((-1,) + (1,) * (len(shape) - position - 1))

    loudness = one(*cuts[0])
    for cut in cuts[1:]:
        loudness = loudness * one(*cut)
    return loudness


def scatter_about(rng, shape, deviation, bound, split=(), held_as=jnp.bfloat16):
    entries = jax.random.normal(rng, shape, jnp.float32) * deviation
    if len(split) > 0:
        entries = shard_levels(rng, shape, split, -0.22, 0.18) * entries
    return jnp.clip(entries, min=-bound, max=bound).astype(held_as)


def setup_inputs(seed: int = 0) -> dict:
    keys = jax.random.split(jax.random.key(seed), 8)
    query = scatter_about(keys[0], (LEN, QH * DH), 1.0, 6.0, ((0, 16), (1, 2)))
    key_rows = scatter_about(keys[1], (LEN, DH), 1.0, 6.0, ((0, 16),))
    value_rows = scatter_about(keys[2], (LEN, DH), 1.0, 6.0, ((0, 16),))
    output = scatter_about(keys[3], (LEN, QH * DH), 0.25, 1.5, ((0, 16), (1, 2)))
    grad_output = scatter_about(keys[4], (LEN, QH * DH), 24.0, 144.0, ((0, 16), (1, 2)))
    log_norm = draw_log_norm(jax.random.fold_in(keys[7], 71), 0)
    stripe = jax.random.permutation(keys[6], N_SEQ).astype(jnp.int32)
    return {"query": query, "key_rows": key_rows, "value_rows": value_rows, "output": output, "grad_output": grad_output, "log_norm": log_norm, "stripe": stripe}


def block_terms(query_heads, grad_heads, lse_rows, delta_rows, key_block, value_block, diag_open):
    extent = key_block.shape[0]
    factor = key_block.shape[1] ** -0.5
    scores = jnp.einsum("shd,td->hst", query_heads, key_block) * factor
    row_ids = lax.broadcasted_iota(jnp.int32, (extent, extent), 0)
    col_ids = lax.broadcasted_iota(jnp.int32, (extent, extent), 1)
    allowed = (col_ids < row_ids) | ((col_ids == row_ids) & diag_open)
    weights = jnp.where(allowed[None], jnp.exp(scores - lse_rows[:, :, None]), jnp.float32(0.0))
    weights_low = lax.optimization_barrier(weights.astype(jnp.bfloat16)).astype(jnp.float32)
    grad_values = jnp.einsum("hst,shd->td", weights_low, grad_heads)
    grad_weights = jnp.einsum("shd,td->hst", grad_heads, value_block)
    grad_scores = (factor * weights * (grad_weights - delta_rows[:, :, None])).astype(jnp.bfloat16)
    grad_scores = lax.optimization_barrier(grad_scores).astype(jnp.float32)
    grad_query = jnp.einsum("hst,td->shd", grad_scores, key_block)
    grad_keys = jnp.einsum("hst,shd->td", grad_scores, query_heads)
    return grad_query, jnp.stack([grad_keys, grad_values])


def reference(query, key_rows, value_rows, output, grad_output, log_norm, stripe):
    query_blocks = query.reshape(N_SEQ, S_DEV, QH, DH)
    grad_blocks = grad_output.reshape(N_SEQ, S_DEV, QH, DH)
    output_blocks = output.reshape(N_SEQ, S_DEV, QH, DH)
    lse_blocks = log_norm.reshape(QH, N_SEQ, S_DEV).transpose(1, 0, 2)
    key_blocks = key_rows.reshape(N_SEQ, S_DEV, DH)
    value_blocks = value_rows.reshape(N_SEQ, S_DEV, DH)

    def one_block(grad_kv, block_index):
        query_heads = query_blocks[block_index].astype(jnp.float32)
        grad_heads = grad_blocks[block_index].astype(jnp.float32)
        delta_rows = jnp.sum(grad_heads * output_blocks[block_index].astype(jnp.float32), axis=2).T
        lse_rows = lse_blocks[block_index]
        grad_query = jnp.zeros((S_DEV, QH, DH), jnp.float32)
        for offset in range(WINDOW):
            source = ((block_index - offset) % N_SEQ).astype(jnp.int32)
            diag_open = stripe[source] <= stripe[block_index]
            key_block = key_blocks[source].astype(jnp.float32)
            value_block = value_blocks[source].astype(jnp.float32)
            query_part, kv_part = block_terms(query_heads, grad_heads, lse_rows, delta_rows, key_block, value_block, diag_open)
            grad_query = grad_query + query_part
            grad_kv = grad_kv.at[source].add(kv_part)
        return grad_kv, grad_query.astype(jnp.bfloat16)

    start_kv = jnp.zeros((N_SEQ, 2, S_DEV, DH), jnp.float32)
    grad_kv, grad_query = lax.scan(one_block, start_kv, jnp.arange(N_SEQ, dtype=jnp.int32))
    grad_key = grad_kv[:, 0].reshape(LEN, DH).astype(jnp.bfloat16)
    grad_value = grad_kv[:, 1].reshape(LEN, DH).astype(jnp.bfloat16)
    return grad_query.reshape(LEN, QH * DH), grad_key, grad_value
```

```python
import functools

import jax
import jax.numpy as jnp
from jax import lax
from jax.experimental import pallas as pl
from jax.experimental.pallas import tpu as pltpu
from jax.sharding import PartitionSpec as P

WINDOW = 8
GROUP = WINDOW // 2
LOG2E = 1.4426950408889634
F32 = jnp.float32
BF16 = jnp.bfloat16
STEPS = ((0, 0), (1, 0), (1, 1), (1, 2), (1, 3), (0, 2), (0, 3), (0, 1))


def dot(a, b, ca, cb):
    return lax.dot_general(a, b, (((ca,), (cb,)), ((), ())), preferred_element_type=F32)


def kernel(
    n, stripe, q_hbm, k_hbm, v_hbm, o_hbm, g_hbm, lse_hbm,
    dq_out, dk_out, dv_out,
    q, g, o, lse, delta, kv, dqt, acc, part, rx, zs, fin,
    in_sem, kv_send, kv_recv, p_send, p_recv, z_send, z_recv,
):
    me = lax.axis_index("seq")
    y = lax.axis_index("head")
    j = lax.rem(me, GROUP)
    base = me - j
    S, D2 = kv.shape[1:]
    D = D2 // 2
    H = q.shape[1] // D
    half = S // 2
    factor = D ** -0.5

    def mate(t):
        low = j % 2
        high = j // 2
        low = (1 - low) if t & 1 else low
        high = (1 - high) if t & 2 else high
        return high * 2 + low

    def at(t):
        return base + mate(t)

    def plane(d):
        return lax.rem(me + d * GROUP + n, n)

    loads = [
        pltpu.make_async_copy(k_hbm, kv.at[j, :, pl.ds(0, D)], in_sem.at[0]),
        pltpu.make_async_copy(v_hbm, kv.at[j, :, pl.ds(D, D)], in_sem.at[1]),
        pltpu.make_async_copy(q_hbm, q, in_sem.at[2]),
        pltpu.make_async_copy(g_hbm, g, in_sem.at[3]),
        pltpu.make_async_copy(o_hbm, o, in_sem.at[4]),
        pltpu.make_async_copy(lse_hbm, lse, in_sem.at[5]),
    ]
    for c in loads:
        c.start()

    barrier = pltpu.get_barrier_semaphore()
    peers = [(at(t), y) for t in (1, 2, 3)] + [(at(t), 1 - y) for t in range(4)]
    peers += [(plane(d), y) for d in (1, -1, 2, -2)]
    for p in peers:
        pl.semaphore_signal(barrier, inc=1, device_id=p, device_id_type=pl.DeviceIdType.MESH)
    loads[0].wait()
    loads[1].wait()
    pl.semaphore_wait(barrier, len(peers))

    A = lambda i: i
    B = lambda i: GROUP + i
    C = 2 * GROUP

    def remote(src, dst, ss, rs, to):
        return pltpu.make_async_remote_copy(
            src_ref=src, dst_ref=dst, send_sem=ss, recv_sem=rs,
            device_id=to, device_id_type=pl.DeviceIdType.MESH,
        )

    def kv_copy(src, dst, sem, to):
        return remote(kv.at[src], kv.at[dst], kv_send.at[sem], kv_recv.at[dst], (to, y))

    up_b = kv_copy(A(j), B(j), 0, plane(1))
    up_c = kv_copy(B(j), C, 1, plane(1))
    own = {t: kv_copy(A(j), A(j), 1 + t, at(t)) for t in (1, 2)}
    late = {t: kv_copy(C, A(j), 1 + t, at(t)) for t in (1, 2)}
    b_out = {t: kv_copy(B(j), B(j), 3 + t, at(t)) for t in (1, 2)}
    b_relay = kv_copy(B(mate(2)), B(mate(2)), 6, at(1))
    a_relay = kv_copy(A(mate(2)), A(mate(2)), 7, at(1))

    def kv_arrived(slot):
        kv_copy(slot, slot, 0, at(1)).wait_recv()

    up_b.start()
    for t in (1, 2):
        pl.when(mate(t) > j)(own[t].start)

    for c in loads[2:]:
        c.wait()

    ones = jnp.ones((8, D), BF16)
    for h in range(H):
        cols = slice(h * D, (h + 1) * D)
        prod = g[:, cols].astype(F32) * o[:, cols].astype(F32)
        hi = prod.astype(BF16)
        rest = prod - hi.astype(F32)
        mid = rest.astype(BF16)
        low = (rest - mid.astype(F32)).astype(BF16)
        total = dot(ones, hi, 1, 1) + dot(ones, mid, 1, 1) + dot(ones, low, 1, 1)
        delta[h] = total
    dqt[...] = jnp.zeros_like(dqt)
    own_stripe = stripe[me]

    rows = lax.broadcasted_iota(jnp.int32, (half, half), 0)
    diff = lax.broadcasted_iota(jnp.int32, (half, half), 1) - rows

    def heads(slot, least, first):
        def one(h):
            cols = pl.ds(pl.multiple_of(h * D, D), D)
            k0, k1 = kv[slot, :half, :D], kv[slot, half:, :D]
            v0, v1 = kv[slot, :half, D:], kv[slot, half:, D:]
            qh, gh = q[:, cols], g[:, cols]
            l2 = lse[pl.ds(h, 1), :] * LOG2E
            dl = delta[h, 0:1, :]
            s0 = dot(k0, qh, 1, 1)
            s1 = dot(k1, qh[half:], 1, 1)
            w0 = dot(v0, gh, 1, 1)
            w1 = dot(v1, gh[half:], 1, 1)
            p0 = jnp.exp2(s0 * (factor * LOG2E) - l2)
            open_ = diff >= least
            p0 = jnp.concatenate([jnp.where(open_, p0[:, :half], 0.0), p0[:, half:]], axis=1)
            p1 = jnp.where(open_, jnp.exp2(s1 * (factor * LOG2E) - l2[:, half:]), 0.0)
            d0 = (p0 * (w0 - dl)).astype(BF16)
            d1 = (p1 * (w1 - dl[:, half:])).astype(BF16)
            dv0 = dot(p0.astype(BF16), gh, 1, 0)
            dv1 = dot(p1.astype(BF16), gh[half:], 1, 0)
            dk0 = dot(d0, qh, 1, 0)
            dk1 = dot(d1, qh[half:], 1, 0)
            dqt[h, :, :] += dot(k0, d0, 0, 0)
            dqt[h, :, half:] += dot(k1, d1, 0, 0)
            return dk0, dv0, dk1, dv1

        return one

    def compute(slot, late_flag, i, between):
        if late_flag:
            source = base - GROUP + i
        else:
            source = base + i - jnp.where(i > j, 2 * GROUP, 0)
        source = lax.rem(source + n, n)
        least = jnp.where(stripe[source] <= own_stripe, 0, 1)
        one = heads(slot, least, True)

        def pair(h0, keep):
            a = one(h0)
            b = one(h0 + 1)
            for m in range(4):
                r, c = m // 2, m % 2
                s = a[m] + b[m]
                if keep:
                    s = s + acc[r, :, c * D:(c + 1) * D]
                acc[r, :, c * D:(c + 1) * D] = s

        pair(0, False)
        between()

        @pl.loop(1, H // 2)
        def _(m):
            pair(2 * m, True)

    def part_copies(step):
        late_flag, t = STEPS[step]
        to = at(t)
        res = []
        if t:
            res.append(remote(part.at[step, y], rx.at[late_flag, t, 0],
                              p_send.at[step, 0], p_recv.at[late_flag, t, 0], (to, y)))
        res.append(remote(part.at[step, 1 - y], rx.at[late_flag, t, 1],
                          p_send.at[step, 1], p_recv.at[late_flag, t, 1], (to, 1 - y)))
        return res

    def send_part(step):
        for c in part_copies(step):
            c.start()

    z_copies = [
        remote(zs.at[m], fin.at[m], z_send.at[m], z_recv.at[m], (plane(-1 - m), y)) for m in range(2)
    ]
    bsteps = {t: STEPS.index((1, t)) for t in range(4)}
    asteps = {t: STEPS.index((0, t)) for t in range(4)}

    def arrived_part(flag, t):
        def get(m):
            remote(rx.at[flag, t, m], rx.at[flag, t, m], p_send.at[0, 0], p_recv.at[flag, t, m],
                   (at(1), y)).wait_recv()
            return rx[flag, t, m].astype(F32)

        first = part[STEPS.index((flag, 0)), y].astype(F32) if t == 0 else get(0)
        return first + get(1)

    for step, (flag, t) in enumerate(STEPS):
        i = mate(t)
        slot = B(i) if flag else A(i)
        if (flag, t) == (1, 0):
            kv_arrived(slot)
            up_c.start()
            b_out[1].start()
            b_out[2].start()
        elif (flag, t) == (1, 2):
            kv_arrived(slot)
            b_relay.start()
            kv_arrived(C)
            for u in (1, 2):
                pl.when(mate(u) < j)(late[u].start)
        elif (flag, t) == (0, 2):
            kv_arrived(slot)
            a_relay.start()
        elif (flag, t) != (0, 0):
            kv_arrived(slot)

        def between():
            if step:
                send_part(step - 1)

        compute(slot, flag, i, between)
        for r in range(2):
            part[step, r] = acc[r].astype(BF16)
        if step == 6:
            total = arrived_part(1, 0)
            for u in (1, 2, 3):
                total = total + arrived_part(1, u)
            zs[0] = total.astype(BF16)

    send_part(len(STEPS) - 1)
    z_copies[0].start()

    for h in range(H):
        dq_out[:, h * D:(h + 1) * D] = (dqt[h] * factor).T.astype(BF16)

    mine = arrived_part(0, 0)
    other = jnp.zeros_like(mine)
    for u in (2, 3, 1):
        x = arrived_part(0, u)
        here = mate(u) > j
        mine = mine + jnp.where(here, x, 0.0)
        other = other + jnp.where(here, 0.0, x)
    zs[1] = other.astype(BF16)
    z_copies[1].start()
    z_copies[0].wait_recv()
    mine = mine + fin[0].astype(F32)
    z_copies[1].wait_recv()
    mine = mine + fin[1].astype(F32)
    dk_out[...] = (mine[:, :D] * factor).astype(BF16)
    dv_out[...] = mine[:, D:].astype(BF16)

    for c in [up_b, up_c, own[1], own[2], b_out[1], b_out[2], b_relay, a_relay]:
        c.wait_send()
    for step in range(len(STEPS)):
        for c in part_copies(step):
            c.wait_send()
    for c in z_copies:
        c.wait_send()


def shards(n, query, key_rows, value_rows, output, grad_output, log_norm, stripe):
    S, W = query.shape
    D = key_rows.shape[1]
    H = W // D
    half = S // 2
    any_ = pl.BlockSpec(memory_space=pl.ANY)
    vm = pl.BlockSpec(memory_space=pltpu.VMEM)
    dma = pltpu.SemaphoreType.DMA
    return pl.pallas_call(
        functools.partial(kernel, n),
        out_shape=(
            jax.ShapeDtypeStruct((S, W), BF16),
            jax.ShapeDtypeStruct((half, D), BF16),
            jax.ShapeDtypeStruct((half, D), BF16),
        ),
        in_specs=[pl.BlockSpec(memory_space=pltpu.SMEM)] + [any_] * 6,
        out_specs=(vm, vm, vm),
        scratch_shapes=[
            pltpu.VMEM((S, W), BF16),
            pltpu.VMEM((S, W), BF16),
            pltpu.VMEM((S, W), BF16),
            pltpu.VMEM((H, S), F32),
            pltpu.VMEM((H, 8, S), F32),
            pltpu.VMEM((2 * GROUP + 1, S, 2 * D), BF16),
            pltpu.VMEM((H, D, S), F32),
            pltpu.VMEM((2, half, 2 * D), F32),
            pltpu.VMEM((len(STEPS), 2, half, 2 * D), BF16),
            pltpu.VMEM((2, GROUP, 2, half, 2 * D), BF16),
            pltpu.VMEM((2, half, 2 * D), BF16),
            pltpu.VMEM((2, half, 2 * D), BF16),
            dma((6,)),
            dma((8,)),
            dma((2 * GROUP + 1,)),
            dma((len(STEPS), 2)),
            dma((2, GROUP, 2)),
            dma((2,)),
            dma((2,)),
        ],
        compiler_params=pltpu.CompilerParams(
            collective_id=0, has_side_effects=True, vmem_limit_bytes=48 * 1024 * 1024
        ),
        name="window_backward",
    )(stripe, query, key_rows, value_rows, output, grad_output, log_norm)


def solution(mesh):
    placed = (
        P("seq", "head"),
        P("seq", None),
        P("seq", None),
        P("seq", "head"),
        P("seq", "head"),
        P("head", "seq"),
        P(),
    )
    return jax.shard_map(
        functools.partial(shards, mesh.shape["seq"]),
        mesh=mesh,
        in_specs=placed,
        out_specs=(P("seq", "head"), P(("seq", "head"), None), P(("seq", "head"), None)),
        check_vma=False,
    )
```

```python
import functools

import jax
import jax.numpy as jnp
from jax import lax
from jax.experimental import pallas as pl
from jax.experimental.pallas import tpu as pltpu
from jax.sharding import PartitionSpec as P

WINDOW = 8
GROUP = WINDOW // 2
LOG2E = 1.4426950408889634
F32 = jnp.float32
BF16 = jnp.bfloat16
STEPS = ((0, 0), (1, 1), (1, 0), (1, 3), (1, 2), (0, 3), (0, 2), (0, 1))
GIVEN = {(1, 1): 0, (1, 3): 1, (0, 3): 2}
TAKEN = {(1, 0): 0, (1, 2): 1, (0, 2): 2}
SENT = ((0, 0), (1, 0), (1, 2), (0, 2), (0, 1))


def dot(a, b, ca, cb):
    return lax.dot_general(a, b, (((ca,), (cb,)), ((), ())), preferred_element_type=F32)


def kernel(
    n, stripe, q_hbm, k_hbm, v_hbm, o_hbm, g_hbm, lse_hbm,
    dq_out, dk_out, dv_out,
    q, g, o, lse, delta, kv, dqt, acc, give, take, part, rx, zs, fin,
    in_sem, kv_send, kv_recv, d_send, d_recv, p_send, p_recv, z_send, z_recv,
):
    me = lax.axis_index("seq")
    y = lax.axis_index("head")
    j = lax.rem(me, GROUP)
    base = me - j
    S, D2 = kv.shape[1:]
    D = D2 // 2
    H = q.shape[1] // D
    half = S // 2
    factor = D ** -0.5

    def mate(t):
        low = j % 2
        high = j // 2
        low = (1 - low) if t & 1 else low
        high = (1 - high) if t & 2 else high
        return high * 2 + low

    def at(t):
        return base + mate(t)

    def plane(d):
        return lax.rem(me + d * GROUP + n, n)

    loads = [
        pltpu.make_async_copy(k_hbm, kv.at[j, :, pl.ds(0, D)], in_sem.at[0]),
        pltpu.make_async_copy(v_hbm, kv.at[j, :, pl.ds(D, D)], in_sem.at[1]),
        pltpu.make_async_copy(q_hbm, q, in_sem.at[2]),
        pltpu.make_async_copy(g_hbm, g, in_sem.at[3]),
        pltpu.make_async_copy(o_hbm, o, in_sem.at[4]),
        pltpu.make_async_copy(lse_hbm, lse, in_sem.at[5]),
    ]
    for c in loads:
        c.start()

    barrier = pltpu.get_barrier_semaphore()
    peers = [(at(t), y) for t in (1, 2, 3)] + [(at(t), 1 - y) for t in range(4)]
    peers += [(plane(d), y) for d in (1, -1, 2, -2)]
    for p in peers:
        pl.semaphore_signal(barrier, inc=1, device_id=p, device_id_type=pl.DeviceIdType.MESH)
    loads[0].wait()
    loads[1].wait()
    pl.semaphore_wait(barrier, len(peers))

    A = lambda i: i
    B = lambda i: GROUP + i
    C = 2 * GROUP

    def remote(src, dst, ss, rs, to):
        return pltpu.make_async_remote_copy(
            src_ref=src, dst_ref=dst, send_sem=ss, recv_sem=rs,
            device_id=to, device_id_type=pl.DeviceIdType.MESH,
        )

    def kv_copy(src, dst, sem, to):
        return remote(kv.at[src], kv.at[dst], kv_send.at[sem], kv_recv.at[dst], (to, y))

    up_b = kv_copy(A(j), B(j), 0, plane(1))
    up_c = kv_copy(B(j), C, 1, plane(1))
    own = {t: kv_copy(A(j), A(j), 1 + t, at(t)) for t in (1, 2)}
    late = {t: kv_copy(C, A(j), 1 + t, at(t)) for t in (1, 2)}
    b_out = {t: kv_copy(B(j), B(j), 3 + t, at(t)) for t in (1, 2)}
    b_relay = kv_copy(B(mate(2)), B(mate(2)), 6, at(1))
    a_relay = kv_copy(A(mate(2)), A(mate(2)), 7, at(1))

    def kv_arrived(slot):
        kv_copy(slot, slot, 0, at(1)).wait_recv()

    up_b.start()
    for t in (1, 2):
        pl.when(mate(t) > j)(own[t].start)

    for c in loads[2:]:
        c.wait()

    ones = jnp.ones((8, D), BF16)
    for h in range(H):
        cols = slice(h * D, (h + 1) * D)
        prod = g[:, cols].astype(F32) * o[:, cols].astype(F32)
        hi = prod.astype(BF16)
        rest = prod - hi.astype(F32)
        mid = rest.astype(BF16)
        low = (rest - mid.astype(F32)).astype(BF16)
        total = dot(ones, hi, 1, 1) + dot(ones, mid, 1, 1) + dot(ones, low, 1, 1)
        delta[h] = total * factor
    dqt[...] = jnp.zeros_like(dqt)
    own_stripe = stripe[me]

    rows = lax.broadcasted_iota(jnp.int32, (half, half), 0)
    diff = lax.broadcasted_iota(jnp.int32, (half, half), 1) - rows

    def heads(slot, least, first):
        def one(h):
            cols = pl.ds(pl.multiple_of(h * D, D), D)
            k0, k1 = kv[slot, :half, :D], kv[slot, half:, :D]
            v0, v1 = kv[slot, :half, D:], kv[slot, half:, D:]
            qh, gh = q[:, cols], g[:, cols]
            l2 = lse[pl.ds(h, 1), :] * LOG2E
            dl = delta[h, 0:1, :]
            s0 = dot(k0, qh, 1, 1)
            s1 = dot(k1, qh[half:], 1, 1)
            w0 = dot(v0, gh, 1, 1)
            w1 = dot(v1, gh[half:], 1, 1)
            p0 = jnp.exp2(s0 * (factor * LOG2E) - l2)
            open_ = diff >= least
            p0 = jnp.concatenate([jnp.where(open_, p0[:, :half], 0.0), p0[:, half:]], axis=1)
            p1 = jnp.where(open_, jnp.exp2(s1 * (factor * LOG2E) - l2[:, half:]), 0.0)
            d0 = (p0 * (w0 * factor - dl)).astype(BF16)
            d1 = (p1 * (w1 * factor - dl[:, half:])).astype(BF16)
            dv0 = dot(p0.astype(BF16), gh, 1, 0)
            dv1 = dot(p1.astype(BF16), gh[half:], 1, 0)
            dk0 = dot(d0, qh, 1, 0)
            dk1 = dot(d1, qh[half:], 1, 0)
            dqt[h, :, :] += dot(k0, d0, 0, 0)
            dqt[h, :, half:] += dot(k1, d1, 0, 0)
            return dk0, dv0, dk1, dv1

        return one

    def compute(slot, late_flag, i, between):
        if late_flag:
            source = base - GROUP + i
        else:
            source = base + i - jnp.where(i > j, 2 * GROUP, 0)
        source = lax.rem(source + n, n)
        least = jnp.where(stripe[source] <= own_stripe, 0, 1)
        one = heads(slot, least, True)

        def pair(h0, keep):
            a = one(h0)
            b = one(h0 + 1)
            for m in range(4):
                r, c = m // 2, m % 2
                s = a[m] + b[m]
                if keep:
                    s = s + acc[r, :, c * D:(c + 1) * D]
                acc[r, :, c * D:(c + 1) * D] = s

        pair(0, False)
        between()

        @pl.loop(1, H // 2)
        def _(m):
            pair(2 * m, True)

    def part_copies(key):
        late_flag, t = key
        to = at(t)
        slot = SENT.index(key)
        res = []
        if t:
            res.append(remote(part.at[slot, y], rx.at[slot, 0],
                              p_send.at[slot, 0], p_recv.at[slot, 0], (to, y)))
        res.append(remote(part.at[slot, 1 - y], rx.at[slot, 1],
                          p_send.at[slot, 1], p_recv.at[slot, 1], (to, 1 - y)))
        return res

    def pair_copy(m):
        return remote(give.at[m], take.at[m], d_send.at[m], d_recv.at[m], (at(1), y))

    def send_part(key):
        if key in GIVEN:
            pair_copy(GIVEN[key]).start()
        else:
            for c in part_copies(key):
                c.start()

    z_copies = [
        remote(zs.at[m], fin.at[m], z_send.at[m], z_recv.at[m], (plane(-1 - m), y)) for m in range(2)
    ]

    def arrived_part(flag, t):
        slot = SENT.index((flag, t))

        def get(m):
            remote(rx.at[slot, m], rx.at[slot, m], p_send.at[0, 0], p_recv.at[slot, m],
                   (at(1), y)).wait_recv()
            return rx[slot, m].astype(F32)

        first = part[slot, y].astype(F32) if t == 0 else get(0)
        return first + get(1)

    for step, (flag, t) in enumerate(STEPS):
        i = mate(t)
        slot = B(i) if flag else A(i)
        if (flag, t) == (1, 1):
            kv_arrived(B(j))
            up_c.start()
            b_out[1].start()
            b_out[2].start()
            kv_arrived(slot)
        elif (flag, t) == (1, 3):
            kv_arrived(B(mate(2)))
            b_relay.start()
            kv_arrived(C)
            for u in (1, 2):
                pl.when(mate(u) < j)(late[u].start)
            kv_arrived(slot)
        elif (flag, t) == (0, 3):
            kv_arrived(A(mate(2)))
            a_relay.start()
            kv_arrived(slot)
        elif (flag, t) == (0, 1):
            kv_arrived(slot)

        def between():
            if step:
                send_part(STEPS[step - 1])
            if step == 7:
                z_copies[0].start()

        compute(slot, flag, i, between)
        key = (flag, t)
        if key in GIVEN:
            give[GIVEN[key]] = acc[...]
        elif key in TAKEN:
            m = TAKEN[key]
            pair_copy(m).wait_recv()
            part[SENT.index(key)] = (acc[...] + take[m]).astype(BF16)
        else:
            part[SENT.index(key)] = acc[...].astype(BF16)
        if step == 6:
            zs[0] = (arrived_part(1, 0) + arrived_part(1, 2)).astype(BF16)

    send_part(STEPS[-1])

    for h in range(H):
        dq_out[:, h * D:(h + 1) * D] = dqt[h].T.astype(BF16)

    mine = arrived_part(0, 0)
    other = jnp.zeros_like(mine)
    for u in (2, 1):
        x = arrived_part(0, u)
        here = mate(u) > j
        mine = mine + jnp.where(here, x, 0.0)
        other = other + jnp.where(here, 0.0, x)
    zs[1] = other.astype(BF16)
    z_copies[1].start()
    z_copies[0].wait_recv()
    mine = mine + fin[0].astype(F32)
    z_copies[1].wait_recv()
    mine = mine + fin[1].astype(F32)
    dk_out[...] = mine[:, :D].astype(BF16)
    dv_out[...] = mine[:, D:].astype(BF16)

    for c in [up_b, up_c, own[1], own[2], b_out[1], b_out[2], b_relay, a_relay]:
        c.wait_send()
    for key in SENT:
        for c in part_copies(key):
            c.wait_send()
    for m in range(len(GIVEN)):
        pair_copy(m).wait_send()
    for c in z_copies:
        c.wait_send()


def shards(n, query, key_rows, value_rows, output, grad_output, log_norm, stripe):
    S, W = query.shape
    D = key_rows.shape[1]
    H = W // D
    half = S // 2
    any_ = pl.BlockSpec(memory_space=pl.ANY)
    vm = pl.BlockSpec(memory_space=pltpu.VMEM)
    dma = pltpu.SemaphoreType.DMA
    return pl.pallas_call(
        functools.partial(kernel, n),
        out_shape=(
            jax.ShapeDtypeStruct((S, W), BF16),
            jax.ShapeDtypeStruct((half, D), BF16),
            jax.ShapeDtypeStruct((half, D), BF16),
        ),
        in_specs=[pl.BlockSpec(memory_space=pltpu.SMEM)] + [any_] * 6,
        out_specs=(vm, vm, vm),
        scratch_shapes=[
            pltpu.VMEM((S, W), BF16),
            pltpu.VMEM((S, W), BF16),
            pltpu.VMEM((S, W), BF16),
            pltpu.VMEM((H, S), F32),
            pltpu.VMEM((H, 8, S), F32),
            pltpu.VMEM((2 * GROUP + 1, S, 2 * D), BF16),
            pltpu.VMEM((H, D, S), F32),
            pltpu.VMEM((2, half, 2 * D), F32),
            pltpu.VMEM((len(GIVEN), 2, half, 2 * D), F32),
            pltpu.VMEM((len(GIVEN), 2, half, 2 * D), F32),
            pltpu.VMEM((len(SENT), 2, half, 2 * D), BF16),
            pltpu.VMEM((len(SENT), 2, half, 2 * D), BF16),
            pltpu.VMEM((2, half, 2 * D), BF16),
            pltpu.VMEM((2, half, 2 * D), BF16),
            dma((6,)),
            dma((8,)),
            dma((2 * GROUP + 1,)),
            dma((len(GIVEN),)),
            dma((len(GIVEN),)),
            dma((len(SENT), 2)),
            dma((len(SENT), 2)),
            dma((2,)),
            dma((2,)),
        ],
        compiler_params=pltpu.CompilerParams(
            collective_id=0, has_side_effects=True, vmem_limit_bytes=67043328
        ),
        name="window_backward",
    )(stripe, query, key_rows, value_rows, output, grad_output, log_norm)


def solution(mesh):
    placed = (
        P("seq", "head"),
        P("seq", None),
        P("seq", None),
        P("seq", "head"),
        P("seq", "head"),
        P("head", "seq"),
        P(),
    )
    return jax.shard_map(
        functools.partial(shards, mesh.shape["seq"]),
        mesh=mesh,
        in_specs=placed,
        out_specs=(P("seq", "head"), P(("seq", "head"), None), P(("seq", "head"), None)),
        check_vma=False,
    )
```
